32 devices in a mesh: grp: 2 (over x), row: 8 (over z, y), col: 2 (over core).
Axes of the slice: x: 2, y: 2, z: 4, core: 2. Of those that a mesh axis runs over, the one named last changes fastest.
Arguments:
- density: bfloat16 [1024, 32, 128], P(('grp', 'row', 'col')), parts along dimension 0, may hold values from -6 to 6
- leaf_target: int32 [1024], P(('grp', 'row', 'col')), parts along dimension 0, may hold values from 0 to 511, as said below
- geometry: float32 [6, 131072], P(None, ('grp', 'row', 'col')), parts along dimension 1, may hold values from -6 to 6
- near_list: int32 [1024, 16], P(('grp', 'row', 'col')), parts along dimension 0, may hold values from -1 to 511, as said below
- far_list: int32 [1024, 16], P(('grp', 'row', 'col')), parts along dimension 0, may hold values from -1 to 511, as said below
- node_list: int32 [128, 32], P(('grp', 'row', 'col')), parts along dimension 0, may hold values from -1 to 63, as said below
- basis_in: bfloat16 [1024, 64, 128], P(('grp', 'row', 'col')), parts along dimension 0, may hold values from -0.5 to 0.5
- basis_out: bfloat16 [1024, 64, 128], P(('grp', 'row', 'col')), parts along dimension 0, may hold values from -0.75 to 0.75
- transfer: bfloat16 [128, 64, 512], P(('grp', 'row', 'col')), parts along dimension 0, may hold values from -0.25 to 0.25
- node_points: float32 [3, 8192], P(None, 'grp'), parts along dimension 1, may hold values from -6 to 6
Outputs:
- potential: bfloat16 [1024, 32, 128], P(('grp', 'row', 'col')), parts along dimension 0
The draws below stay inside these ranges and needn't reach their ends.
There are 2 independent parts, one for each index of `grp`. The reference program is written for one: setup_inputs(seed, part) draws one part's arguments, and reference() takes and returns one part's arrays. A program takes and returns all parts, laid end to end along the dimension named above; each array names one. Nothing has to cross between parts.
Inputs may be any that keep to these rules, and one draw needn't show every extreme that they name: `leaf_target`: A permutation of the tree positions; of the 32 slab leaves of one device, exactly 2 go to the block of 32 tree positions of each device. `near_list`: row t holds t in slot 0; every other slot holds either -1 or a leaf other than t within 16 of t, the leaves of a row distinct; a -1 may stand in any slot after slot 0, also between leaves. `far_list`: every slot of row t holds either -1 or a leaf within 16 of t that is neither t nor in row t of near_list, the leaves of a row distinct; a -1 may stand in any slot, also between leaves. `node_list`: row p holds distinct nodes that differ from p by more than 2, then -1 in the unused slots.
All inputs are finite; a program needn't handle non-finite values.
Results may differ from the reference program's by a relative error of at most 0.0053.
Values may be sent and summed in bfloat16 or wider, within the bound.
A program may use at most 64 MiB of HBM per device.

```python
import math
import jax
import jax.numpy as jnp
from jax import lax

LEAF = 128
RANK = 64
NRHS = 32
CHILD = 8
REACH = 16
NEAR = 16
FAR = 16
FAR_NODE = 32
LEAF_DEV = 32
LEAVES = 512
PANELS = 65536
NODES = 64


def draw_leaf_target(key, part):
    shards = LEAVES // LEAF_DEV
    per_peer = LEAF_DEV // shards
    first_key, second_key = jax.random.split(jax.random.fold_in(key, 11))
    sender_order = jax.vmap(lambda item: jax.random.permutation(item, LEAF_DEV))(jax.random.split(first_key, shards))
    receiver_order = jax.vmap(lambda item: jax.random.permutation(item, LEAF_DEV))(jax.random.split(second_key, shards))
    sender_ids = jnp.arange(shards, dtype=jnp.int32)[:, None, None]
    receiver_ids = jnp.arange(shards, dtype=jnp.int32)[None, :, None]
    slab_pos = sender_ids * LEAF_DEV + sender_order.reshape(shards, shards, per_peer).astype(jnp.int32)
    tree_pos = receiver_ids * LEAF_DEV + receiver_order.reshape(shards, shards, per_peer).transpose(1, 0, 2).astype(jnp.int32)
    return jnp.zeros((LEAVES,), jnp.int32).at[slab_pos.reshape(-1)].set(tree_pos.reshape(-1))


def leaf_lists(key):
    first_key, second_key, third_key = jax.random.split(jax.random.fold_in(key, 5), 3)
    offsets = jnp.concatenate([jnp.arange(-REACH, 0), jnp.arange(1, REACH + 1)]).astype(jnp.int32)
    order = jax.vmap(lambda item: jax.random.permutation(item, 2 * REACH))(jax.random.split(first_key, LEAVES))
    chosen = offsets[order]
    target = jnp.arange(LEAVES, dtype=jnp.int32)[:, None]
    source = target + chosen
    inside = (source >= 0) & (source < LEAVES)
    near_live = jax.random.randint(second_key, (LEAVES, 1), NEAR // 4, NEAR)
    far_live = jax.random.randint(third_key, (LEAVES, 1), FAR // 2, FAR + 1)
    near_keep = inside[:, :NEAR - 1] & (jnp.arange(NEAR - 1)[None, :] < near_live)
    near_rows = jnp.concatenate([target, jnp.where(near_keep, source[:, :NEAR - 1], -1)], axis=1)
    far_keep = inside[:, NEAR - 1:NEAR - 1 + FAR] & (jnp.arange(FAR)[None, :] < far_live)
    far_rows = jnp.where(far_keep, source[:, NEAR - 1:NEAR - 1 + FAR], -1)
    return (near_rows.astype(jnp.int32), far_rows.astype(jnp.int32))


def draw_near_list(key, part):
    return leaf_lists(key)[0]


def draw_far_list(key, part):
    return leaf_lists(key)[1]


def draw_node_list(key, part):
    first_key, second_key = jax.random.split(jax.random.fold_in(key, 9))
    order = jax.vmap(lambda item: jax.random.permutation(item, NODES))(jax.random.split(first_key, NODES)).astype(jnp.int32)
    owner = jnp.arange(NODES, dtype=jnp.int32)[:, None]
    closeby = (jnp.abs(order - owner) <= 2).astype(jnp.int32)
    places = jnp.argsort(closeby, axis=1, stable=True)[:, :FAR_NODE]
    picked = jnp.take_along_axis(order, places, axis=1)
    live_count = jax.random.randint(second_key, (NODES, 1), FAR_NODE // 2, FAR_NODE + 1)
    return jnp.where(jnp.arange(FAR_NODE)[None, :] < live_count, picked, -1).astype(jnp.int32)


def steps_of(stream_key, shape, cuts, low, largest):
    loudness, own = 1.0, jax.random.fold_in(stream_key, 6)
    for dim, shards_of in cuts:
        draws = jnp.exp(jax.random.uniform(jax.random.fold_in(own, dim), (shards_of,), jnp.float32, low / len(cuts), largest / len(cuts)))
        loudness = loudness * jnp.repeat(draws, shape[dim] // shards_of).reshape([-1 if axis == dim else 1 for axis in range(len(shape))])
    return loudness


def normal_values(own_key, shape, width, limit, cuts=(), kind=jnp.bfloat16):
    level = steps_of(own_key, shape, cuts, -0.22, 0.18) if cuts else 1.0
    result = jax.random.normal(own_key, shape, jnp.float32) * width * level
    return jnp.minimum(jnp.maximum(result, -limit), limit).astype(kind)


def setup_inputs(seed: int = 0, part: int = 0) -> dict:
    arg_keys = jax.random.split(jax.random.key(seed), 11)
    part_keys = jax.random.split(jax.random.fold_in(arg_keys[10], part), 11)
    density = normal_values(part_keys[0], (LEAVES, NRHS, LEAF), 1.0, 6.0, ((0, 16),))
    leaf_target = draw_leaf_target(jax.random.fold_in(jax.random.fold_in(arg_keys[10], part), 71), part)
    geometry = normal_values(part_keys[2], (6, PANELS), 1.0, 6.0, ((1, 16),), jnp.float32)
    near_list = draw_near_list(jax.random.fold_in(jax.random.fold_in(arg_keys[10], part), 71), part)
    far_list = draw_far_list(jax.random.fold_in(jax.random.fold_in(arg_keys[10], part), 71), part)
    node_list = draw_node_list(jax.random.fold_in(jax.random.fold_in(arg_keys[10], part), 71), part)
    basis_in = normal_values(part_keys[6], (LEAVES, RANK, LEAF), LEAF ** -0.5, 0.5, ((0, 16),))
    basis_out = normal_values(part_keys[7], (LEAVES, RANK, LEAF), RANK ** -0.5, 0.75, ((0, 16),))
    transfer = normal_values(part_keys[8], (NODES, RANK, CHILD * RANK), (CHILD * RANK) ** -0.5, 0.25, ((0, 16),))
    node_points = normal_values(part_keys[9], (3, NODES * RANK), 1.0, 6.0, (), jnp.float32)
    return {"density": density, "leaf_target": leaf_target, "geometry": geometry, "near_list": near_list, "far_list": far_list, "node_list": node_list, "basis_in": basis_in, "basis_out": basis_out, "transfer": transfer, "node_points": node_points}


smoothing = 0.1
inv_four_pi = 0.25 / math.pi

def coupling(targets, sources):
    spread = targets - sources
    return inv_four_pi / jnp.sqrt(lax.optimization_barrier(jnp.sum(spread * spread, axis=0)) + smoothing * smoothing)

def double_layer(targets, sources, normals):
    spread = targets - sources
    distance = lax.optimization_barrier(jnp.sum(spread * spread, axis=0)) + smoothing * smoothing
    return inv_four_pi * lax.optimization_barrier(jnp.sum(normals * spread, axis=0)) / (distance * jnp.sqrt(distance))

def reference(density, leaf_target, geometry, near_list, far_list, node_list, basis_in, basis_out, transfer, node_points):
    source_rows = jnp.argsort(leaf_target).astype(jnp.int32)
    ordered = density[source_rows]
    skeleton = jnp.einsum('tnl,trl->tnr', ordered.astype(jnp.float32), basis_in.astype(jnp.float32)).astype(jnp.bfloat16)
    stacked = skeleton.reshape(NODES, CHILD, NRHS, RANK).transpose(0, 2, 1, 3).reshape(NODES, NRHS, CHILD * RANK)
    node_skel = jnp.einsum('pnk,prk->pnr', stacked.astype(jnp.float32), transfer.astype(jnp.float32)).astype(jnp.bfloat16)
    shaped = geometry.reshape(6, LEAVES, LEAF)
    proxies = shaped[0:3, :, :RANK]
    node_pts = node_points.reshape(3, NODES, RANK)
    leaf_ids = jnp.arange(LEAVES, dtype=jnp.int32)
    node_ids = jnp.arange(NODES, dtype=jnp.int32)
    zero_half = jnp.zeros((), jnp.bfloat16)

    def leaf_far_block(packed):
        target_ids, entries = packed
        usable = entries >= 0
        sources = jnp.where(usable, entries, 0)
        weights = coupling(proxies[:, target_ids][:, :, None, :, None], proxies[:, sources][:, :, :, None, :]).astype(jnp.bfloat16)
        skel_src = jnp.where(usable[:, :, None, None], skeleton[sources], zero_half)
        return jnp.einsum('bsij,bsnj->bni', weights.astype(jnp.float32), skel_src.astype(jnp.float32))
    leaf_far = lax.map(leaf_far_block, (leaf_ids.reshape(-1, 16), far_list.reshape(-1, 16, FAR))).reshape(LEAVES, NRHS, RANK)

    def node_far_block(packed):
        target_ids, entries = packed
        usable = entries >= 0
        sources = jnp.where(usable, entries, 0)
        weights = coupling(node_pts[:, target_ids][:, :, None, :, None], node_pts[:, sources][:, :, :, None, :]).astype(jnp.bfloat16)
        skel_src = jnp.where(usable[:, :, None, None], node_skel[sources], zero_half)
        return jnp.einsum('bsij,bsnj->bni', weights.astype(jnp.float32), skel_src.astype(jnp.float32))
    node_far = lax.map(node_far_block, (node_ids.reshape(-1, 8), node_list.reshape(-1, 8, FAR_NODE))).reshape(NODES, NRHS, RANK).astype(jnp.bfloat16)
    down = jnp.einsum('pnr,prk->pnk', node_far.astype(jnp.float32), transfer.astype(jnp.float32))
    down = down.reshape(NODES, NRHS, CHILD, RANK).transpose(0, 2, 1, 3).reshape(LEAVES, NRHS, RANK)
    local = (leaf_far + down).astype(jnp.bfloat16)
    far_out = jnp.einsum('tnr,trl->tnl', local.astype(jnp.float32), basis_out.astype(jnp.float32))

    def near_block(packed):
        target_ids, entries = packed
        usable = entries >= 0
        sources = jnp.where(usable, entries, 0)
        source_geo = shaped[:, sources]
        kernel = double_layer(shaped[0:3, target_ids][:, :, None, :, None], source_geo[0:3][:, :, :, None, :], source_geo[3:6][:, :, :, None, :]).astype(jnp.bfloat16)
        dens_src = jnp.where(usable[:, :, None, None], ordered[sources], zero_half)
        return jnp.einsum('bsij,bsnj->bni', kernel.astype(jnp.float32), dens_src.astype(jnp.float32))
    near_out = lax.map(near_block, (leaf_ids.reshape(-1, 16), near_list.reshape(-1, 16, NEAR))).reshape(LEAVES, NRHS, LEAF)
    return (near_out + far_out).astype(jnp.bfloat16)
```

```python
import functools
import math

import jax
import jax.numpy as jnp
from jax import lax
from jax.experimental import pallas as pl
from jax.experimental.pallas import tpu as pltpu
from jax.sharding import PartitionSpec as P

REACH = 16
smoothing = 0.1
inv_four_pi = 0.25 / math.pi
NT = (((1,), (1,)), ((), ()))
bf16, f32 = jnp.bfloat16, jnp.float32
EARLY, MIDDLE = 8, 16


def thirds(a):
    high = a.astype(bf16).astype(f32)
    rest = a - high
    mid = rest.astype(bf16).astype(f32)
    return high, mid, rest - mid


def left_side(a):
    h, m, l = thirds(a)
    return jnp.concatenate([h, m, h, l, h, m], axis=0)


def right_side(a):
    h, m, l = thirds(a)
    return jnp.concatenate([h, h, m, h, l, m], axis=0)


def xyz_square(points, row):
    xyz = jnp.where(row < 3, points, 0.0)
    return xyz, jnp.sum(xyz * xyz, axis=0, keepdims=True)


def target_form(points, row):
    _, square = xyz_square(points, row)
    return jnp.where(row < 3, points, jnp.where(row == 3, square, jnp.where(row == 4, 1.0, 0.0)))


def source_form(points, row):
    xyz, square = xyz_square(points, row)
    return xyz, jnp.where(
        row < 3,
        -2.0 * points,
        jnp.where(row == 3, 1.0, jnp.where(row == 4, square + smoothing * smoothing, 0.0)),
    )


def each(lo, hi, group, body):
    while (hi - lo) % group:
        group //= 2

    def step(i, carry):
        for k in range(group):
            body(lo + i * group + k)
        return carry

    lax.fori_loop(0, (hi - lo) // group, step, 0)


def whole_kernel(
    picks, slots, near_list, far_list, node_list, density, geo, node_pts, basis_in_far, transfer_far,
    basis_out_far, out,
    basis_in, transfer, basis_out, local_sem, outgoing, slot_rows, arrived, arrived_rows, geo_wide, dens_wide,
    skel_wide, all_skel, near_src, near_tgt, far_src, far_tgt, far_skel, near_k, far_k, down, send_sem, recv_sem,
):
    leaves, nrhs, size = out.shape
    here, rank, width = transfer.shape
    children = width // rank
    wide = leaves + 2 * REACH
    rows_n, cols_n = lax.axis_size("row"), lax.axis_size("col")
    count = rows_n * cols_n
    per = leaves // count
    nodes = count * here
    base = wide + 1
    my_row, my_col = lax.axis_index("row"), lax.axis_index("col")
    me = my_row * cols_n + my_col
    first_leaf = me * leaves
    inner = geo.shape[1]
    halo = REACH * size
    row = lax.broadcasted_iota(jnp.int32, (8, size), 0)
    lane = lax.broadcasted_iota(jnp.int32, (1, size), 1)
    low = lane < rank

    def peer(k):
        q = lax.rem(me + k, count)
        return q, {"row": q // cols_n, "col": lax.rem(q, cols_n)}

    copies = []

    def send(src, dst, where):
        k = len(copies)
        copy = pltpu.make_async_remote_copy(
            src_ref=src, dst_ref=dst, send_sem=send_sem.at[k], recv_sem=recv_sem.at[k],
            device_id=where, device_id_type=pl.DeviceIdType.MESH,
        )
        copy.start()
        copies.append(copy)
        return copy

    def columns(ref, block):
        return ref[:, pl.ds(pl.multiple_of(block * size, size), size)]

    barrier = pltpu.get_barrier_semaphore()
    for k in range(1, count):
        pl.semaphore_signal(barrier, inc=1, device_id=peer(k)[1], device_id_type=pl.DeviceIdType.MESH)
    fetches = []
    for k, (src, dst) in enumerate(
        ((basis_in_far, basis_in), (transfer_far, transfer), (basis_out_far, basis_out))
    ):
        fetch = pltpu.make_async_copy(src, dst, local_sem.at[k])
        fetch.start()
        fetches.append(fetch)

    for j in range(leaves):
        outgoing[j] = density[jnp.clip(picks[j], 0, leaves - 1)]
    for q in range(count):
        line = jnp.zeros((1, size), jnp.int32)
        for k in range(per):
            line = line + jnp.where(lane == slots[q * per + k], me * per + k + 1, 0)
        slot_rows[q] = line
    geo_wide[0:6, halo : halo + inner] = geo[...]

    def turned(form):
        rest = jnp.zeros((size - form.shape[0], size), f32)
        return jnp.concatenate([form, rest], axis=0).T

    def store_far_source(index, low_form):
        far_src[0, index] = low_form.astype(bf16)
        far_src[1, index] = pltpu.roll(low_form, rank, 1).astype(bf16)

    def node_block(b):
        _, source = source_form(
            jnp.concatenate([columns(node_pts, b), jnp.zeros((5, size), f32)], axis=0), row
        )
        form = turned(right_side(source))
        store_far_source(base + 2 * b, form[:rank])
        store_far_source(base + 2 * b + 1, form[rank:])

    each(0, nodes // 2, 4, node_block)

    pl.semaphore_wait(barrier, count - 1)
    geo_copies = [
        send(geo.at[:, pl.ds(inner - halo, halo)], geo_wide.at[pl.ds(0, 6), pl.ds(0, halo)], peer(1)[1]),
        send(geo.at[:, pl.ds(0, halo)], geo_wide.at[pl.ds(0, 6), pl.ds(halo + inner, halo)], peer(count - 1)[1]),
    ]
    exchange = []
    for k in range(1, count):
        q, where = peer(k)
        exchange.append(send(slot_rows.at[q], arrived_rows.at[me], where))
        exchange.append(
            send(outgoing.at[pl.ds(q * per, per)], arrived.at[pl.ds(me * per, per)], where)
        )
    arrived_rows[me] = slot_rows[me]
    for k in range(per):
        arrived[me * per + k] = outgoing[me * per + k]

    def store_far_target(index, low_form, high_form):
        gap = jnp.zeros((rank - low_form.shape[0], size), f32)
        none = jnp.zeros((2 * rank, size), f32)
        block = jnp.concatenate([low_form, gap, high_form, gap], axis=0)
        far_tgt[index] = jnp.concatenate(
            [jnp.concatenate([block, none], axis=0), jnp.concatenate([none, block], axis=0)], axis=1
        ).astype(bf16)

    def target_block(t):
        form = left_side(target_form(columns(geo_wide, t + REACH), row))
        terms = form.shape[0]
        near_tgt[t] = jnp.concatenate(
            [
                jnp.concatenate([form, jnp.zeros((size - terms, size), f32)], axis=0),
                jnp.concatenate(
                    [jnp.zeros((terms, size), f32), form, jnp.zeros((size - 2 * terms, size), f32)], axis=0
                ),
            ],
            axis=1,
        ).astype(bf16)
        store_far_target(t, jnp.where(low, form, 0.0), jnp.where(low, 0.0, pltpu.roll(form, rank, 1)))

    def source_block(s):
        points = columns(geo_wide, s)
        xyz, source = source_form(points, row)
        normal = jnp.where(row < 3, pltpu.roll(points, 5, 0), 0.0) * inv_four_pi
        shift = -jnp.sum(normal * xyz, axis=0, keepdims=True)
        normal = jnp.where(row == 4, shift, normal)
        left = right_side(source)
        form = turned(jnp.concatenate([left, right_side(normal)], axis=0))
        near_src[s] = form.astype(bf16)
        store_far_source(s, jnp.where(lane < left.shape[0], form[:rank], 0.0))

    each(0, leaves, 4, target_block)
    for b in range(here // 2):
        form = left_side(
            target_form(
                jnp.concatenate(
                    [columns(node_pts, me * (here // 2) + b), jnp.zeros((5, size), f32)], axis=0
                ),
                row,
            )
        )
        other = pltpu.roll(form, rank, 1)
        store_far_target(leaves + 2 * b, jnp.where(low, form, 0.0), jnp.where(low, 0.0, other))
        store_far_target(leaves + 2 * b + 1, jnp.where(low, other, 0.0), jnp.where(low, 0.0, form))
    each(REACH, REACH + leaves, 4, source_block)
    for copy in geo_copies:
        copy.wait_recv()
    each(0, REACH, 4, source_block)
    each(REACH + leaves, wide, 4, source_block)

    def within(entry, shift, pad, least, end):
        return jnp.where(entry < 0, pad, jnp.clip(entry + shift, least, end - 1))

    def near_place(t, k, pad):
        return within(near_list[t, k], REACH - first_leaf, pad, 0, wide)

    def far_place(t, k, pad):
        return within(far_list[t, k], REACH - first_leaf, pad, 0, wide)

    def node_place(p, k, pad):
        return within(node_list[p, k], base, pad, base - 1, base + nodes)

    def couple(weights, ids, store):
        for g in range(len(ids) // 4):
            i = ids[4 * g : 4 * g + 4]
            points = jnp.concatenate(
                [far_src[0, i[0]] + far_src[1, i[1]], far_src[0, i[2]] + far_src[1, i[3]]], axis=1
            )
            square = jnp.dot(points, weights, preferred_element_type=f32)
            store(g, (inv_four_pi * lax.rsqrt(square)).astype(bf16))

    far_slots, node_slots = far_list.shape[1], node_list.shape[1]
    per_tile = 16
    tiles = node_slots // per_tile

    def couple_leaf(t):
        def store(g, value):
            far_k[t, g * rank : (g + 1) * rank] = value

        couple(far_tgt[t], [far_place(t, k, t + REACH) for k in range(far_slots)], store)

    def couple_node(p):
        def store(g, value):
            tile, part = g // 4, g % 4
            far_k[leaves + p * tiles + tile, part * rank : (part + 1) * rank] = value

        own = base + me * here + p
        couple(far_tgt[leaves + p], [node_place(p, k, own) for k in range(node_slots)], store)

    each(0, here, 2, couple_node)
    each(0, leaves, 4, couple_leaf)

    near_slots = near_list.shape[1]

    def near_leaf(t):
        weights = near_tgt[t]
        for k in range(near_slots):
            both = jnp.dot(near_src[near_place(t, k, t + REACH)], weights, preferred_element_type=f32)
            r = lax.rsqrt(both[:, :size])
            near_k[t, k * size : (k + 1) * size] = (both[:, size:] * (r * r * r)).astype(bf16)

    each(0, EARLY, 4, near_leaf)

    for copy in exchange:
        copy.wait_recv()
    place = arrived_rows[0]
    for q in range(1, count):
        place = place + arrived_rows[q]
    for s in range(leaves):
        source = jnp.max(jnp.where(lane == s, place, 0)) - 1
        dens_wide[REACH + s] = arrived[jnp.clip(source, 0, leaves - 1)]
    dens_wide[wide] = jnp.zeros((nrhs, size), bf16)
    for fetch in fetches[:2]:
        fetch.wait()

    def skeleton(i):
        pair = [
            lax.dot_general(
                dens_wide[REACH + 2 * i + c], basis_in[2 * i + c], NT, preferred_element_type=f32
            )
            for c in range(2)
        ]
        skel_wide[REACH // 2 + i] = jnp.concatenate(pair, axis=1).astype(bf16)

    each(0, leaves // 2, 4, skeleton)
    second = [
        send(dens_wide.at[pl.ds(leaves, REACH)], dens_wide.at[pl.ds(0, REACH)], peer(1)[1]),
        send(dens_wide.at[pl.ds(REACH, REACH)], dens_wide.at[pl.ds(REACH + leaves, REACH)], peer(count - 1)[1]),
    ]
    pairs_here = here // 2
    for b in range(pairs_here):
        pair = []
        for c in range(2):
            p = 2 * b + c
            first = REACH // 2 + p * children // 2
            stacked = jnp.concatenate([skel_wide[first + j] for j in range(children // 2)], axis=1)
            pair.append(lax.dot_general(stacked, transfer[p], NT, preferred_element_type=f32))
        all_skel[me * pairs_here + b] = jnp.concatenate(pair, axis=1).astype(bf16)
    half = REACH // 2
    second += [
        send(skel_wide.at[pl.ds(leaves // 2, half)], skel_wide.at[pl.ds(0, half)], peer(1)[1]),
        send(skel_wide.at[pl.ds(half, half)], skel_wide.at[pl.ds(half + leaves // 2, half)], peer(count - 1)[1]),
    ]

    def block_of(r, c):
        return all_skel.at[pl.ds((r * cols_n + c) * pairs_here, pairs_here)]

    mine = block_of(my_row, my_col)
    partners = [{"col": lax.rem(my_col + c, cols_n)} for c in range(1, cols_n)]
    along = [
        send(mine, mine, {"row": lax.rem(my_row + k, rows_n)}) for k in range(1, rows_n)
    ]
    second += [send(mine, mine, where) for where in partners]

    each(EARLY, MIDDLE, 4, near_leaf)
    for k in range(1, rows_n):
        along[k - 1].wait_recv()
        block = block_of(lax.rem(my_row + rows_n - k, rows_n), my_col)
        second += [send(block, block, where) for where in partners]
    each(MIDDLE, leaves, 4, near_leaf)
    for copy in second:
        copy.wait_recv()

    def spread(tile, index):
        other = jnp.concatenate([tile[:, rank:], tile[:, :rank]], axis=1)
        none = jnp.zeros_like(tile)
        far_skel[0, index] = jnp.where(low, tile, none)
        far_skel[1, index] = jnp.where(low, none, other)
        far_skel[0, index + 1] = jnp.where(low, other, none)
        far_skel[1, index + 1] = jnp.where(low, none, tile)

    each(0, nodes // 2, 4, lambda i: spread(all_skel[i], base + 2 * i))
    each(0, wide // 2, 4, lambda i: spread(skel_wide[i], 2 * i))
    for v in range(2):
        far_skel[v, wide] = jnp.zeros((nrhs, size), bf16)
    fetches[2].wait()

    def gathered(ids, matrix):
        lines = []
        for p in range(4):
            i = [ids[4 * g + p] for g in range(4)]
            lines.append(
                jnp.concatenate(
                    [far_skel[0, i[0]] + far_skel[1, i[1]], far_skel[0, i[2]] + far_skel[1, i[3]]], axis=1
                )
            )
        result = jnp.dot(jnp.concatenate(lines, axis=0), matrix, preferred_element_type=f32)
        even = result[:nrhs, :size] + result[2 * nrhs : 3 * nrhs, size:]
        odd = result[nrhs : 2 * nrhs, :size] + result[3 * nrhs :, size:]
        return (even + pltpu.roll(odd, rank, 1))[:, :rank]

    for p in range(here):
        ids = [node_place(p, k, wide) for k in range(node_slots)]
        far = sum(
            gathered(ids[i * per_tile : (i + 1) * per_tile], far_k[leaves + p * tiles + i])
            for i in range(tiles)
        ).astype(bf16)
        spreading = jnp.dot(far, transfer[p], preferred_element_type=f32)
        for c in range(children):
            down[p * children + c] = spreading[:, c * rank : (c + 1) * rank]

    def finish(t):
        far = gathered([far_place(t, k, wide) for k in range(far_slots)], far_k[t])
        charge = jnp.concatenate([dens_wide[near_place(t, k, wide)] for k in range(near_slots)], axis=1)
        near = jnp.dot(charge, near_k[t], preferred_element_type=f32)
        local = (far + down[t]).astype(bf16)
        out[t] = (near + jnp.dot(local, basis_out[t], preferred_element_type=f32)).astype(bf16)

    each(0, leaves, 4, finish)
    for copy in copies:
        copy.wait_send()


def on_device(
    density, leaf_target, geometry, near_list, far_list, node_list, basis_in, basis_out, transfer, node_points,
):
    leaves, nrhs, size = density.shape
    rank = basis_in.shape[1]
    here = transfer.shape[0]
    wide = leaves + 2 * REACH
    rows_n, cols_n = lax.axis_size("row"), lax.axis_size("col")
    count = rows_n * cols_n
    nodes = here * count
    per = leaves // count
    destination = leaf_target // leaves
    ids = jnp.arange(leaves, dtype=jnp.int32)
    earlier = (destination[:, None] == destination) & (ids[:, None] > ids)
    order = destination * per + jnp.sum(earlier.astype(jnp.int32), axis=1)
    placed = order == ids[:, None]
    picks = jnp.sum(jnp.where(placed, ids, 0), axis=1)
    slots = jnp.sum(jnp.where(placed, leaf_target % leaves, 0), axis=1)
    tiles = node_list.shape[1] // 16
    n_copies = 2 * (count - 1) + 2 + 4 + (rows_n - 1) + (cols_n - 1) + (rows_n - 1) * (cols_n - 1)
    smem = pl.BlockSpec(memory_space=pltpu.SMEM)
    vmem = pl.BlockSpec(memory_space=pltpu.VMEM)
    away = pl.BlockSpec(memory_space=pl.ANY)
    return pl.pallas_call(
        whole_kernel,
        out_shape=jax.ShapeDtypeStruct((leaves, nrhs, size), bf16),
        in_specs=[smem] * 5 + [vmem] * 3 + [away] * 3,
        out_specs=vmem,
        scratch_shapes=[
            pltpu.VMEM(basis_in.shape, bf16),
            pltpu.VMEM(transfer.shape, bf16),
            pltpu.VMEM(basis_out.shape, bf16),
            pltpu.SemaphoreType.DMA((3,)),
            pltpu.VMEM((leaves, nrhs, size), bf16),
            pltpu.VMEM((count, 1, size), jnp.int32),
            pltpu.VMEM((leaves, nrhs, size), bf16),
            pltpu.VMEM((count, 1, size), jnp.int32),
            pltpu.VMEM((8, wide * size), f32),
            pltpu.VMEM((wide + 1, nrhs, size), bf16),
            pltpu.VMEM((wide // 2, nrhs, size), bf16),
            pltpu.VMEM((nodes // 2, nrhs, size), bf16),
            pltpu.VMEM((wide, size, size), bf16),
            pltpu.VMEM((leaves, size, 2 * size), bf16),
            pltpu.VMEM((2, wide + 1 + nodes, rank, size), bf16),
            pltpu.VMEM((leaves + here, 4 * rank, 4 * rank), bf16),
            pltpu.VMEM((2, wide + 1 + nodes, nrhs, size), bf16),
            pltpu.VMEM((leaves, near_list.shape[1] * size, size), bf16),
            pltpu.VMEM((leaves + here * tiles, 4 * rank, 4 * rank), bf16),
            pltpu.VMEM((leaves, nrhs, rank), f32),
            pltpu.SemaphoreType.DMA((n_copies,)),
            pltpu.SemaphoreType.DMA((n_copies,)),
        ],
        compiler_params=pltpu.CompilerParams(
            collective_id=0, has_side_effects=True, vmem_limit_bytes=58 * 1024 * 1024
        ),
        name="whole",
    )(
        picks, slots, near_list, far_list, node_list, density, geometry, node_points, basis_in, transfer,
        basis_out,
    )


def solution(mesh):
    leaf = ("grp", "row", "col")
    return jax.shard_map(
        on_device,
        mesh=mesh,
        in_specs=(
            P(leaf, None, None), P(leaf), P(None, leaf), P(leaf, None), P(leaf, None), P(leaf, None),
            P(leaf, None, None), P(leaf, None, None), P(leaf, None, None), P(None, "grp"),
        ),
        out_specs=P(leaf, None, None),
        check_vma=False,
    )
```

```python
import functools
import math

import jax
import jax.numpy as jnp
from jax import lax
from jax.experimental import pallas as pl
from jax.experimental.pallas import tpu as pltpu
from jax.sharding import PartitionSpec as P

REACH = 16
smoothing = 0.1
inv_four_pi = 0.25 / math.pi
NT = (((1,), (1,)), ((), ()))
bf16, f32 = jnp.bfloat16, jnp.float32
EARLY, MIDDLE = 0, 20


def thirds(a):
    high = a.astype(bf16).astype(f32)
    rest = a - high
    mid = rest.astype(bf16).astype(f32)
    return high, mid, rest - mid


def left_side(a):
    h, m, l = thirds(a)
    return jnp.concatenate([h, m, h, l, h, m], axis=0)


def right_side(a):
    h, m, l = thirds(a)
    return jnp.concatenate([h, h, m, h, l, m], axis=0)


def xyz_square(points, row):
    xyz = jnp.where(row < 3, points, 0.0)
    return xyz, jnp.sum(xyz * xyz, axis=0, keepdims=True)


def target_form(points, row):
    _, square = xyz_square(points, row)
    return jnp.where(row < 3, points, jnp.where(row == 3, square, jnp.where(row == 4, 1.0, 0.0)))


def source_form(points, row):
    xyz, square = xyz_square(points, row)
    return xyz, jnp.where(
        row < 3,
        -2.0 * points,
        jnp.where(row == 3, 1.0, jnp.where(row == 4, square + smoothing * smoothing, 0.0)),
    )


def each(lo, hi, group, body):
    if hi <= lo:
        return
    while (hi - lo) % group:
        group //= 2

    def step(i, carry):
        for k in range(group):
            body(lo + i * group + k)
        return carry

    lax.fori_loop(0, (hi - lo) // group, step, 0)


def whole_kernel(
    near_list, far_list, node_list, leaf_target, density, geo, node_pts, basis_in_far, transfer_far,
    basis_out_far, out,
    basis_in, transfer, local_sem, outgoing, slot_rows, arrived, arrived_rows, geo_wide, dens_wide,
    skel_wide, all_skel, near_src, near_tgt, far_src, far_tgt, far_skel, near_k, far_k, down, local, send_sem, recv_sem,
):
    leaves, nrhs, size = out.shape
    here, rank, width = transfer.shape
    children = width // rank
    wide = leaves + 2 * REACH
    rows_n, cols_n = lax.axis_size("row"), lax.axis_size("col")
    count = rows_n * cols_n
    per = leaves // count
    nodes = count * here
    base = wide + 1
    my_row, my_col = lax.axis_index("row"), lax.axis_index("col")
    me = my_row * cols_n + my_col
    first_leaf = me * leaves
    inner = geo.shape[1]
    halo = REACH * size
    row = lax.broadcasted_iota(jnp.int32, (8, size), 0)
    lane = lax.broadcasted_iota(jnp.int32, (1, size), 1)
    low = lane < rank

    def peer(k):
        q = lax.rem(me + k, count)
        return q, {"row": q // cols_n, "col": lax.rem(q, cols_n)}

    copies = []

    def send(src, dst, where):
        k = len(copies)
        copy = pltpu.make_async_remote_copy(
            src_ref=src, dst_ref=dst, send_sem=send_sem.at[k], recv_sem=recv_sem.at[k],
            device_id=where, device_id_type=pl.DeviceIdType.MESH,
        )
        copy.start()
        copies.append(copy)
        return copy

    def columns(ref, block):
        return ref[:, pl.ds(pl.multiple_of(block * size, size), size)]

    near_slots, far_slots, node_slots = near_list.shape[0], far_list.shape[0], node_list.shape[1]
    near_rows = near_slots * size
    barrier = pltpu.get_barrier_semaphore()
    for k in range(1, count):
        pl.semaphore_signal(barrier, inc=1, device_id=peer(k)[1], device_id_type=pl.DeviceIdType.MESH)
    fetches = []
    for k, (src, dst) in enumerate(
        ((basis_in_far, basis_in), (transfer_far, transfer), (basis_out_far, near_k.at[:, pl.ds(near_rows, rank)]))
    ):
        fetch = pltpu.make_async_copy(src, dst, local_sem.at[k])
        fetch.start()
        fetches.append(fetch)

    shift = leaves.bit_length() - 1
    target = leaf_target[...]
    leaf_row = lax.broadcasted_iota(jnp.int32, (leaves, leaves), 0)
    leaf_col = lax.broadcasted_iota(jnp.int32, (leaves, leaves), 1)
    target_down = jnp.sum(jnp.where(leaf_row == leaf_col, target, 0), axis=1, keepdims=True)
    owner, owner_down = target >> shift, target_down >> shift
    earlier = jnp.where((owner_down == owner) & (leaf_row > leaf_col), 1, 0)
    rank_down = jnp.sum(earlier, axis=1, keepdims=True)
    picks = jnp.sum(jnp.where(owner_down * per + rank_down == leaf_col, leaf_row, 0), axis=0, keepdims=True)
    slot_hit = (target_down & (leaves - 1)) == lane
    mark = jnp.where(slot_hit, me * per + rank_down + 1, 0)
    for q in range(count):
        slot_rows[q] = jnp.sum(jnp.where(owner_down == q, mark, 0), axis=0, keepdims=True)
    for j in range(leaves):
        pick = jnp.max(jnp.where(leaf_col[:1] == j, picks, 0))
        outgoing[j] = density[jnp.clip(pick, 0, leaves - 1)]
    geo_wide[0:6, halo : halo + inner] = geo[...]

    def turned(form):
        rest = jnp.zeros((size - form.shape[0], size), f32)
        return jnp.concatenate([form, rest], axis=0).T

    def store_far_source(index, low_form):
        far_src[0, index] = low_form.astype(bf16)
        far_src[1, index] = pltpu.roll(low_form, rank, 1).astype(bf16)

    def node_block(b):
        _, source = source_form(
            jnp.concatenate([columns(node_pts, b), jnp.zeros((5, size), f32)], axis=0), row
        )
        form = turned(right_side(source))
        store_far_source(base + 2 * b, form[:rank])
        store_far_source(base + 2 * b + 1, form[rank:])

    each(0, nodes // 2, 4, node_block)

    def store_far_target(index, low_form, high_form):
        gap = jnp.zeros((rank - low_form.shape[0], size), f32)
        none = jnp.zeros((2 * rank, size), f32)
        block = jnp.concatenate([low_form, gap, high_form, gap], axis=0)
        far_tgt[index] = jnp.concatenate(
            [jnp.concatenate([block, none], axis=0), jnp.concatenate([none, block], axis=0)], axis=1
        ).astype(bf16)

    def target_block(t):
        form = left_side(target_form(columns(geo_wide, t + REACH), row))
        terms = form.shape[0]
        near_tgt[t] = jnp.concatenate(
            [
                jnp.concatenate([form, jnp.zeros((size - terms, size), f32)], axis=0),
                jnp.concatenate(
                    [jnp.zeros((terms, size), f32), form, jnp.zeros((size - 2 * terms, size), f32)], axis=0
                ),
            ],
            axis=1,
        ).astype(bf16)
        store_far_target(t, jnp.where(low, form, 0.0), jnp.where(low, 0.0, pltpu.roll(form, rank, 1)))

    def source_block(s):
        points = columns(geo_wide, s)
        xyz, source = source_form(points, row)
        normal = jnp.where(row < 3, pltpu.roll(points, 5, 0), 0.0) * inv_four_pi
        shift = -jnp.sum(normal * xyz, axis=0, keepdims=True)
        normal = jnp.where(row == 4, shift, normal)
        left = right_side(source)
        form = turned(jnp.concatenate([left, right_side(normal)], axis=0))
        near_src[s] = form.astype(bf16)
        store_far_source(s, jnp.where(lane < left.shape[0], form[:rank], 0.0))

    each(0, leaves, 4, target_block)
    for b in range(here // 2):
        form = left_side(
            target_form(
                jnp.concatenate(
                    [columns(node_pts, me * (here // 2) + b), jnp.zeros((5, size), f32)], axis=0
                ),
                row,
            )
        )
        other = pltpu.roll(form, rank, 1)
        store_far_target(leaves + 2 * b, jnp.where(low, form, 0.0), jnp.where(low, 0.0, other))
        store_far_target(leaves + 2 * b + 1, jnp.where(low, other, 0.0), jnp.where(low, 0.0, form))
    each(REACH, REACH + leaves, 4, source_block)
    pl.semaphore_wait(barrier, count - 1)
    geo_copies = [
        send(geo.at[:, pl.ds(inner - halo, halo)], geo_wide.at[pl.ds(0, 6), pl.ds(0, halo)], peer(1)[1]),
        send(geo.at[:, pl.ds(0, halo)], geo_wide.at[pl.ds(0, 6), pl.ds(halo + inner, halo)], peer(count - 1)[1]),
    ]
    exchange = []
    for k in range(1, count):
        q, where = peer(k)
        exchange.append(send(slot_rows.at[q], arrived_rows.at[me], where))
        exchange.append(
            send(outgoing.at[pl.ds(q * per, per)], arrived.at[pl.ds(me * per, per)], where)
        )
    arrived_rows[me] = slot_rows[me]
    for k in range(per):
        arrived[me * per + k] = outgoing[me * per + k]

    def within(entry, shift, pad, least, end):
        return jnp.where(entry < 0, pad, jnp.clip(entry + shift, least, end - 1))

    def near_place(t, k, pad):
        return within(near_list[k, t], REACH - first_leaf, pad, 0, wide)

    def far_place(t, k, pad):
        return within(far_list[k, t], REACH - first_leaf, pad, 0, wide)

    def node_place(p, k, pad):
        return within(node_list[p, k], base, pad, base - 1, base + nodes)

    def couple(weights, ids, store):
        for g in range(len(ids) // 4):
            i = ids[4 * g : 4 * g + 4]
            points = jnp.concatenate(
                [far_src[0, i[0]] + far_src[1, i[1]], far_src[0, i[2]] + far_src[1, i[3]]], axis=1
            )
            square = jnp.dot(points, weights, preferred_element_type=f32)
            store(g, (inv_four_pi * lax.rsqrt(square)).astype(bf16))

    per_tile = 16
    tiles = node_slots // per_tile

    def couple_leaf(t):
        def store(g, value):
            far_k[t, g * rank : (g + 1) * rank] = value

        couple(far_tgt[t], [far_place(t, k, t + REACH) for k in range(far_slots)], store)

    def couple_node(p):
        def store(g, value):
            tile, part = g // 4, g % 4
            far_k[leaves + p * tiles + tile, part * rank : (part + 1) * rank] = value

        own = base + me * here + p
        couple(far_tgt[leaves + p], [node_place(p, k, own) for k in range(node_slots)], store)

    each(0, here, 2, couple_node)
    for copy in geo_copies:
        copy.wait_recv()
    each(0, REACH, 4, source_block)
    each(REACH + leaves, wide, 4, source_block)
    each(0, leaves, 8, couple_leaf)

    def near_leaf(t):
        weights = near_tgt[t]
        for k in range(near_slots):
            both = jnp.dot(near_src[near_place(t, k, t + REACH)], weights, preferred_element_type=f32)
            r = lax.rsqrt(both[:, :size])
            near_k[t, k * size : (k + 1) * size] = (both[:, size:] * (r * r * r)).astype(bf16)

    each(0, EARLY, 4, near_leaf)

    for copy in exchange:
        copy.wait_recv()
    place = arrived_rows[0]
    for q in range(1, count):
        place = place + arrived_rows[q]
    for s in range(leaves):
        source = jnp.max(jnp.where(lane == s, place, 0)) - 1
        dens_wide[REACH + s] = arrived[jnp.clip(source, 0, leaves - 1)]
    dens_wide[wide] = jnp.zeros((nrhs, size), bf16)
    for fetch in fetches[:2]:
        fetch.wait()

    def skeleton(i):
        pair = [
            lax.dot_general(
                dens_wide[REACH + 2 * i + c], basis_in[2 * i + c], NT, preferred_element_type=f32
            )
            for c in range(2)
        ]
        skel_wide[REACH // 2 + i] = jnp.concatenate(pair, axis=1).astype(bf16)

    each(0, leaves // 2, 4, skeleton)
    second = [
        send(dens_wide.at[pl.ds(leaves, REACH)], dens_wide.at[pl.ds(0, REACH)], peer(1)[1]),
        send(dens_wide.at[pl.ds(REACH, REACH)], dens_wide.at[pl.ds(REACH + leaves, REACH)], peer(count - 1)[1]),
    ]
    pairs_here = here // 2
    for b in range(pairs_here):
        pair = []
        for c in range(2):
            p = 2 * b + c
            first = REACH // 2 + p * children // 2
            stacked = jnp.concatenate([skel_wide[first + j] for j in range(children // 2)], axis=1)
            pair.append(lax.dot_general(stacked, transfer[p], NT, preferred_element_type=f32))
        all_skel[me * pairs_here + b] = jnp.concatenate(pair, axis=1).astype(bf16)
    half = REACH // 2
    second += [
        send(skel_wide.at[pl.ds(leaves // 2, half)], skel_wide.at[pl.ds(0, half)], peer(1)[1]),
        send(skel_wide.at[pl.ds(half, half)], skel_wide.at[pl.ds(half + leaves // 2, half)], peer(count - 1)[1]),
    ]

    def block_of(r, c):
        return all_skel.at[pl.ds((r * cols_n + c) * pairs_here, pairs_here)]

    mine = block_of(my_row, my_col)
    partners = [{"col": lax.rem(my_col + c, cols_n)} for c in range(1, cols_n)]
    along = [
        send(mine, mine, {"row": lax.rem(my_row + k, rows_n)}) for k in range(1, rows_n)
    ]
    second += [send(mine, mine, where) for where in partners]

    each(EARLY, MIDDLE, 4, near_leaf)
    for k in range(1, rows_n):
        along[k - 1].wait_recv()
        block = block_of(lax.rem(my_row + rows_n - k, rows_n), my_col)
        second += [send(block, block, where) for where in partners]
    each(MIDDLE, leaves, 4, near_leaf)
    for copy in second:
        copy.wait_recv()

    def spread(tile, index):
        other = jnp.concatenate([tile[:, rank:], tile[:, :rank]], axis=1)
        none = jnp.zeros_like(tile)
        far_skel[0, index] = jnp.where(low, tile, none)
        far_skel[1, index] = jnp.where(low, none, other)
        far_skel[0, index + 1] = jnp.where(low, other, none)
        far_skel[1, index + 1] = jnp.where(low, none, tile)

    each(0, nodes // 2, 4, lambda i: spread(all_skel[i], base + 2 * i))
    each(0, wide // 2, 4, lambda i: spread(skel_wide[i], 2 * i))
    for v in range(2):
        far_skel[v, wide] = jnp.zeros((nrhs, size), bf16)
    fetches[2].wait()

    def gathered(ids, matrix):
        lines = []
        for p in range(4):
            i = [ids[4 * g + p] for g in range(4)]
            lines.append(
                jnp.concatenate(
                    [far_skel[0, i[0]] + far_skel[1, i[1]], far_skel[0, i[2]] + far_skel[1, i[3]]], axis=1
                )
            )
        result = jnp.dot(jnp.concatenate(lines, axis=0), matrix, preferred_element_type=f32)
        even = result[:nrhs, :size] + result[2 * nrhs : 3 * nrhs, size:]
        odd = result[nrhs : 2 * nrhs, :size] + result[3 * nrhs :, size:]
        return (even + pltpu.roll(odd, rank, 1))[:, :rank]

    for p in range(here):
        ids = [node_place(p, k, wide) for k in range(node_slots)]
        far = sum(
            gathered(ids[i * per_tile : (i + 1) * per_tile], far_k[leaves + p * tiles + i])
            for i in range(tiles)
        ).astype(bf16)
        spreading = jnp.dot(far, transfer[p], preferred_element_type=f32)
        for c in range(children):
            down[p * children + c] = spreading[:, c * rank : (c + 1) * rank]

    def finish_far(t):
        far = gathered([far_place(t, k, wide) for k in range(far_slots)], far_k[t])
        local[t] = (far + down[t]).astype(bf16)

    each(0, leaves, 8, finish_far)

    def finish(t):
        charge = jnp.concatenate(
            [dens_wide[near_place(t, k, wide)] for k in range(near_slots)] + [local[t]], axis=1
        )
        out[t] = jnp.dot(charge, near_k[t], preferred_element_type=f32).astype(bf16)

    each(0, leaves, 8, finish)
    for copy in copies:
        copy.wait_send()


def on_device(
    density, leaf_target, geometry, near_list, far_list, node_list, basis_in, basis_out, transfer, node_points,
):
    leaves, nrhs, size = density.shape
    rank = basis_in.shape[1]
    here = transfer.shape[0]
    wide = leaves + 2 * REACH
    rows_n, cols_n = lax.axis_size("row"), lax.axis_size("col")
    count = rows_n * cols_n
    nodes = here * count
    tiles = node_list.shape[1] // 16
    n_copies = 2 * (count - 1) + 2 + 4 + (rows_n - 1) + (cols_n - 1) + (rows_n - 1) * (cols_n - 1)
    smem = pl.BlockSpec(memory_space=pltpu.SMEM)
    vmem = pl.BlockSpec(memory_space=pltpu.VMEM)
    away = pl.BlockSpec(memory_space=pl.ANY)
    return pl.pallas_call(
        whole_kernel,
        out_shape=jax.ShapeDtypeStruct((leaves, nrhs, size), bf16),
        in_specs=[smem] * 3 + [vmem] * 4 + [away] * 3,
        out_specs=vmem,
        scratch_shapes=[
            pltpu.VMEM(basis_in.shape, bf16),
            pltpu.VMEM(transfer.shape, bf16),
            pltpu.SemaphoreType.DMA((3,)),
            pltpu.VMEM((leaves, nrhs, size), bf16),
            pltpu.VMEM((count, 1, size), jnp.int32),
            pltpu.VMEM((leaves, nrhs, size), bf16),
            pltpu.VMEM((count, 1, size), jnp.int32),
            pltpu.VMEM((8, wide * size), f32),
            pltpu.VMEM((wide + 1, nrhs, size), bf16),
            pltpu.VMEM((wide // 2, nrhs, size), bf16),
            pltpu.VMEM((nodes // 2, nrhs, size), bf16),
            pltpu.VMEM((wide, size, size), bf16),
            pltpu.VMEM((leaves, size, 2 * size), bf16),
            pltpu.VMEM((2, wide + 1 + nodes, rank, size), bf16),
            pltpu.VMEM((leaves + here, 4 * rank, 4 * rank), bf16),
            pltpu.VMEM((2, wide + 1 + nodes, nrhs, size), bf16),
            pltpu.VMEM((leaves, near_list.shape[1] * size + rank, size), bf16),
            pltpu.VMEM((leaves + here * tiles, 4 * rank, 4 * rank), bf16),
            pltpu.VMEM((leaves, nrhs, rank), f32),
            pltpu.VMEM((leaves, nrhs, rank), bf16),
            pltpu.SemaphoreType.DMA((n_copies,)),
            pltpu.SemaphoreType.DMA((n_copies,)),
        ],
        compiler_params=pltpu.CompilerParams(
            collective_id=0, has_side_effects=True, vmem_limit_bytes=58 * 1024 * 1024
        ),
        name="whole",
    )(
        near_list.T, far_list.T, node_list, leaf_target.reshape(1, leaves), density, geometry, node_points,
        basis_in, transfer, basis_out,
    )


def solution(mesh):
    leaf = ("grp", "row", "col")
    return jax.shard_map(
        on_device,
        mesh=mesh,
        in_specs=(
            P(leaf, None, None), P(leaf), P(None, leaf), P(leaf, None), P(leaf, None), P(leaf, None),
            P(leaf, None, None), P(leaf, None, None), P(leaf, None, None), P(None, "grp"),
        ),
        out_specs=P(leaf, None, None),
        check_vma=False,
    )
```
